128 devices in a mesh: img: 1, cfg: 64 (over z, y, x), patch: 2 (over core).
Axes of the slice: x: 4, y: 4, z: 4, core: 2. Of those that a mesh axis runs over, the one named last changes fastest.
Arguments:
- latent: bfloat16 [32, 512, 384], P('img', 'patch')
- cond_vec: float32 [64, 2, 384], P(('img', 'cfg'))
- sched_coef: float32 [3, 2], replicated
- w_ada: bfloat16 [12, 384, 2304], replicated
- w_qkv: bfloat16 [12, 384, 1152], replicated
- w_out: bfloat16 [12, 6, 64, 384], replicated
- w_up: bfloat16 [12, 384, 1536], replicated
- w_down: bfloat16 [12, 1536, 384], replicated
- w_head: bfloat16 [384, 384], replicated
- k_stale: bfloat16 [64, 12, 512, 384], P(('img', 'cfg'))
- v_stale: bfloat16 [64, 12, 512, 384], P(('img', 'cfg'))
Outputs:
- output 1: float32 [64, 512, 384], P(('img', 'cfg'), 'patch')
- output 2: bfloat16 [64, 12, 512, 384], P(('img', 'cfg'))
- output 3: bfloat16 [64, 12, 512, 384], P(('img', 'cfg'))
All inputs are finite; a program needn't handle non-finite values.
Results may differ from the reference program's by a relative error of at most 0.0175248.
Values are sent between devices in bfloat16 or wider.
A program may use at most 1 GiB of HBM per device.

```python
import math
import jax
import jax.numpy as jnp
from jax import lax

D = 384
HEADS = 6
ROWS = 256
LAYERS = 12
N_PATCH = 2
N_PAIRS = 32
N_STEPS = 2

TOKENS = ROWS * N_PATCH
N_SLOTS = 2 * N_PAIRS
HEAD_DIM = D // HEADS
QK_GAIN = (math.sqrt(math.log(TOKENS / 8.0)) / 1.3) ** 0.5
KEY_STD = QK_GAIN * 1.15


def setup_inputs(seed: int = 0, part: int = 0) -> dict:
    root_key = jax.random.key(seed)
    shared_keys = jax.random.split(root_key, 7)
    local_keys = jax.random.split(jax.random.fold_in(root_key, part), 4)
    inv_width = D ** -0.5
    ada_cols = jnp.repeat(jnp.array([0.7, 0.7, 1.7, 0.7, 0.7, 1.7], jnp.float32), D)
    qkv_cols = jnp.repeat(jnp.array([QK_GAIN, QK_GAIN, 1.0], jnp.float32), D)
    w_ada = jax.random.normal(shared_keys[0], (LAYERS, D, 6 * D), jnp.float32) * (ada_cols * inv_width)
    w_qkv = jax.random.normal(shared_keys[1], (LAYERS, D, 3 * D), jnp.float32) * (qkv_cols * inv_width)
    w_out = jax.random.normal(shared_keys[2], (LAYERS, HEADS, HEAD_DIM, D), jnp.float32) * inv_width
    w_up = jax.random.normal(shared_keys[3], (LAYERS, D, 4 * D), jnp.float32) * inv_width
    w_down = jax.random.normal(shared_keys[4], (LAYERS, 4 * D, D), jnp.float32) * (4 * D) ** -0.5
    w_head = jax.random.normal(shared_keys[5], (D, D), jnp.float32) * inv_width
    low_end = jnp.array([0.75, 0.2, 1.5], jnp.float32)[:, None]
    high_end = jnp.array([0.95, 0.4, 3.5], jnp.float32)[:, None]
    sched_coef = low_end + (high_end - low_end) * jax.random.uniform(shared_keys[6], (3, N_STEPS), jnp.float32)
    latent = jax.random.normal(local_keys[0], (N_PAIRS, TOKENS, D), jnp.float32)
    cond_vec = jax.random.normal(local_keys[1], (N_SLOTS, N_STEPS, D), jnp.float32)
    k_stale = jax.random.normal(local_keys[2], (N_SLOTS, LAYERS, TOKENS, D), jnp.float32) * KEY_STD
    v_stale = jax.random.normal(local_keys[3], (N_SLOTS, LAYERS, TOKENS, D), jnp.float32)
    return {
        "latent": latent.astype(jnp.bfloat16),
        "cond_vec": cond_vec,
        "sched_coef": sched_coef,
        "w_ada": w_ada.astype(jnp.bfloat16),
        "w_qkv": w_qkv.astype(jnp.bfloat16),
        "w_out": w_out.astype(jnp.bfloat16),
        "w_up": w_up.astype(jnp.bfloat16),
        "w_down": w_down.astype(jnp.bfloat16),
        "w_head": w_head.astype(jnp.bfloat16),
        "k_stale": k_stale.astype(jnp.bfloat16),
        "v_stale": v_stale.astype(jnp.bfloat16),
    }


def layer_norm(values):
    row_mean = jnp.mean(values, -1, keepdims=True)
    centered = values - row_mean
    row_var = jnp.mean(centered * centered, -1, keepdims=True)
    return centered * lax.rsqrt(row_var + 1e-6)


def attend(queries, key_set, value_set):
    q_blk = min(ROWS, 128)
    blocks = queries.reshape(ROWS // q_blk, q_blk, HEADS, HEAD_DIM).astype(jnp.float32)
    key_h = key_set.reshape(TOKENS, HEADS, HEAD_DIM).astype(jnp.float32)
    val_h = value_set.reshape(TOKENS, HEADS, HEAD_DIM).astype(jnp.float32)
    score_scale = HEAD_DIM ** -0.5

    def one_block(q_part):
        scores = jnp.einsum("qhe,khe->hqk", q_part, key_h) * score_scale
        row_max = jnp.max(scores, -1, keepdims=True)
        weights = jnp.exp(scores - row_max)
        row_sum = jnp.sum(weights, -1)
        mixed_out = jnp.einsum("hqk,khe->qhe", weights.astype(jnp.bfloat16).astype(jnp.float32), val_h)
        return (mixed_out / row_sum.T[:, :, None]).astype(jnp.bfloat16)

    return lax.map(one_block, blocks).reshape(ROWS, HEADS, HEAD_DIM)


def dit_block(resid_now, mod_now, qkv_layer, out_layer, up_layer, down_layer, k_old, v_old):
    shift_attn, scale_attn, gate_attn, shift_mlp, scale_mlp, gate_mlp = jnp.split(mod_now, 6)
    norm_attn = (layer_norm(resid_now) * (1.0 + scale_attn) + shift_attn).astype(jnp.bfloat16)
    qkv_all = jnp.dot(norm_attn, qkv_layer, preferred_element_type=jnp.float32).astype(jnp.bfloat16)
    q_new, k_new, v_new = jnp.split(qkv_all, 3, axis=-1)

    def per_patch(patch_pos):
        row_start = patch_pos * ROWS
        key_set = lax.dynamic_update_slice(k_old, lax.dynamic_slice_in_dim(k_new, row_start, ROWS), (row_start, 0))
        value_set = lax.dynamic_update_slice(v_old, lax.dynamic_slice_in_dim(v_new, row_start, ROWS), (row_start, 0))
        return attend(lax.dynamic_slice_in_dim(q_new, row_start, ROWS), key_set, value_set)

    heads_out = lax.map(per_patch, jnp.arange(N_PATCH)).reshape(TOKENS, HEADS, HEAD_DIM)
    attn_out = jnp.einsum("nhe,hed->nd", heads_out.astype(jnp.float32), out_layer.astype(jnp.float32))
    resid_now = resid_now + gate_attn * attn_out
    norm_mlp = (layer_norm(resid_now) * (1.0 + scale_mlp) + shift_mlp).astype(jnp.bfloat16)
    mlp_up = jnp.dot(norm_mlp, up_layer, preferred_element_type=jnp.float32)
    mlp_act = jax.nn.gelu(mlp_up, approximate=True).astype(jnp.bfloat16)
    mlp_down = jnp.dot(mlp_act, down_layer, preferred_element_type=jnp.float32)
    resid_now = resid_now + gate_mlp * mlp_down
    return resid_now, k_new, v_new


def reference(latent, cond_vec, sched_coef, w_ada, w_qkv, w_out, w_up, w_down, w_head, k_stale, v_stale):
    def one_slot(slot_in):
        img_latent, silu_slot, k_slot, v_slot = slot_in

        def layer_body(resid_now, layer_in):
            ada_layer, qkv_layer, out_layer, up_layer, down_layer, k_old, v_old = layer_in
            mod_now = jnp.dot(silu_slot, ada_layer, preferred_element_type=jnp.float32)
            resid_now, k_new, v_new = dit_block(resid_now, mod_now, qkv_layer, out_layer, up_layer, down_layer, k_old, v_old)
            return resid_now, (k_new, v_new)

        resid_now, fresh_kv = lax.scan(layer_body, img_latent, (w_ada, w_qkv, w_out, w_up, w_down, k_slot, v_slot))
        eps_own = jnp.dot(layer_norm(resid_now).astype(jnp.bfloat16), w_head, preferred_element_type=jnp.float32).astype(jnp.bfloat16)
        return eps_own, fresh_kv[0], fresh_kv[1]

    latent_now = latent.astype(jnp.float32)
    silu_all = jax.nn.silu(cond_vec).astype(jnp.bfloat16)
    k_cache = k_stale
    v_cache = v_stale
    for step_idx in range(N_STEPS):
        slot_in = (jnp.repeat(latent_now, 2, axis=0), silu_all[:, step_idx], k_cache, v_cache)
        eps_own, k_cache, v_cache = lax.map(one_slot, slot_in)
        eps_pairs = eps_own.astype(jnp.float32).reshape(N_PAIRS, 2, TOKENS, D)
        eps_cond = eps_pairs[:, 0]
        eps_unc = eps_pairs[:, 1]
        guided = eps_unc + sched_coef[2, step_idx] * (eps_cond - eps_unc)
        latent_now = sched_coef[0, step_idx] * latent_now + sched_coef[1, step_idx] * guided
    return jnp.repeat(latent_now, 2, axis=0), k_cache, v_cache
```

```python
import functools
import math

import jax
import jax.numpy as jnp
from jax import lax
from jax.experimental import pallas as pl
from jax.experimental.pallas import tpu as pltpu
from jax.sharding import PartitionSpec as P

MESH = pl.DeviceIdType.MESH
F32 = jnp.float32
BF16 = jnp.bfloat16
GELU_A = math.sqrt(2.0 / math.pi)
GELU_B = GELU_A * 0.044715


def normed(values):
    row_mean = jnp.mean(values, -1, keepdims=True)
    centered = values - row_mean
    row_var = jnp.mean(centered * centered, -1, keepdims=True)
    return centered * lax.rsqrt(row_var + 1e-6)


def gelu(x):
    half = 0.5 * x
    return half + half * jnp.tanh(x * (GELU_A + GELU_B * (x * x)))


def contract(a, b, a_dim, b_dim):
    return lax.dot_general(a, b, (((a_dim,), (b_dim,)), ((), ())), preferred_element_type=F32)


def kernel(
    n_steps, n_layers, n_heads, head_dim,
    latent_hbm, cond_ref, sched_ref, ada_ref, qkv_ref, out_ref, up_ref, down_ref, head_ref, k_stale, v_stale,
    x_out, k_out, v_out,
    lat_buf, resid, mod_buf, o_buf, kv_own, kv_peer, eps_send, eps_recv,
    lat_sem, stale_sem, send_sem, recv_sem, last_sem, keep_sem, eps_send_sem, eps_recv_sem,
):
    step = pl.program_id(0)
    layer = pl.program_id(1)
    rows, width = resid.shape
    patch = lax.axis_index("patch")
    slot = lax.axis_index("cfg")
    other = 1 - patch
    partner = slot + 1 - 2 * (slot % 2)
    my_rows = pl.ds(pl.multiple_of(patch * rows, rows), rows)
    peer_rows = pl.ds(pl.multiple_of(other * rows, rows), rows)
    own = (step * n_layers + layer) % 2
    last_step = n_steps - 1
    first = (step == 0) & (layer == 0)

    def load_stale(at_layer):
        place = n_layers + at_layer % 2
        return [
            pltpu.make_async_copy(src.at[0, at_layer, peer_rows], kv_peer.at[place, part], stale_sem.at[at_layer % 2, part])
            for part, src in enumerate((k_stale, v_stale))
        ]

    def send_fresh(at_layer, at_slot):
        return [
            pltpu.make_async_remote_copy(
                src_ref=kv_own.at[at_slot, part], dst_ref=kv_peer.at[at_layer, part],
                send_sem=send_sem.at[at_slot, part], recv_sem=recv_sem.at[at_layer, part],
                device_id={"patch": other}, device_id_type=MESH)
            for part in range(2)
        ]

    def send_final(at_layer, at_slot):
        return [
            pltpu.make_async_remote_copy(
                src_ref=kv_own.at[at_slot, part], dst_ref=dst.at[0, at_layer, my_rows],
                send_sem=send_sem.at[at_slot, part], recv_sem=last_sem.at[at_layer, part],
                device_id={"patch": other}, device_id_type=MESH)
            for part, dst in enumerate((k_out, v_out))
        ]

    def keep_final(at_layer, at_slot):
        return [
            pltpu.make_async_copy(kv_own.at[at_slot, part], dst.at[0, at_layer, my_rows], keep_sem.at[at_slot, part])
            for part, dst in enumerate((k_out, v_out))
        ]

    def send_eps():
        return pltpu.make_async_remote_copy(
            src_ref=eps_send, dst_ref=eps_recv.at[step],
            send_sem=eps_send_sem, recv_sem=eps_recv_sem.at[step],
            device_id={"cfg": partner}, device_id_type=MESH)

    @pl.when(first)
    def _():
        barrier = pltpu.get_barrier_semaphore()
        pl.semaphore_signal(barrier, inc=1, device_id={"patch": other}, device_id_type=MESH)
        pl.semaphore_signal(barrier, inc=1, device_id={"cfg": partner}, device_id_type=MESH)
        fetch = pltpu.make_async_copy(latent_hbm.at[slot // 2], lat_buf, lat_sem)
        fetch.start()
        for copy in load_stale(0):
            copy.start()
        fetch.wait()
        x_out[0] = lat_buf[...].astype(F32)
        pl.semaphore_wait(barrier, 2)

    @pl.when(step == 0)
    def _():
        cond = cond_ref[0]
        act = (cond * jax.nn.sigmoid(cond)).astype(BF16)
        mod_buf[layer, 0:n_steps, :] = jnp.dot(act, ada_ref[0], preferred_element_type=F32)

        for copy in load_stale(layer):
            copy.wait()

        @pl.when(layer + 1 < n_layers)
        def _():
            for copy in load_stale(layer + 1):
                copy.start()

    @pl.when(step > 0)
    def _():
        for copy in send_fresh(layer, own):
            copy.wait_recv()

    @pl.when(layer == 0)
    def _():
        resid[...] = x_out[0]

    def mod(part):
        return mod_buf[layer, pl.ds(step, 1), part * width:(part + 1) * width]

    h = (normed(resid[...]) * (1.0 + mod(1)) + mod(0)).astype(BF16)
    qkv = jnp.dot(h, qkv_ref[0], preferred_element_type=F32).astype(BF16)

    @pl.when((step > 0) | (layer >= 2))
    def _():
        for copy in send_fresh(layer, own):
            copy.wait_send()

    @pl.when((step == last_step) & (layer >= 2))
    def _():
        for copy in keep_final(layer, own):
            copy.wait()

    kv_own[own, 0] = qkv[:, width:2 * width]
    kv_own[own, 1] = qkv[:, 2 * width:]

    place = jnp.where(step == 0, n_layers + layer % 2, layer)
    factor = head_dim ** -0.5 * math.log2(math.e)
    pair_width = 2 * head_dim
    lane = lax.broadcasted_iota(jnp.int32, (rows, pair_width), 1)
    for pair in range(n_heads // 2):
        cols = slice(pair * pair_width, (pair + 1) * pair_width)
        q_pair = qkv[:, cols]
        k_mine = kv_own[own, 0, :, cols]
        k_peer = kv_peer[place, 0, :, cols]
        v_mine = kv_own[own, 1, :, cols].T
        v_peer = kv_peer[place, 1, :, cols].T
        for sub in range(2):
            keep = (lane < head_dim) if sub == 0 else (lane >= head_dim)
            q_head = jnp.where(keep, q_pair, jnp.zeros_like(q_pair))
            s_mine = contract(k_mine, q_head, 1, 1)
            s_peer = contract(k_peer, q_head, 1, 1)
            top = jnp.maximum(jnp.max(s_mine, 0, keepdims=True), jnp.max(s_peer, 0, keepdims=True))
            e_mine = jnp.exp2((s_mine - top) * factor)
            e_peer = jnp.exp2((s_peer - top) * factor)
            total = jnp.sum(e_mine, 0, keepdims=True) + jnp.sum(e_peer, 0, keepdims=True)
            part = slice(sub * head_dim, (sub + 1) * head_dim)
            mixed = contract(v_mine[part], e_mine.astype(BF16), 1, 0) + contract(v_peer[part], e_peer.astype(BF16), 1, 0)
            base = (2 * pair + sub) * head_dim
            o_buf[base:base + head_dim, :] = (mixed * (1.0 / total)).astype(BF16)

    attn = contract(o_buf[...], out_ref[0], 0, 0)
    r = resid[...] + mod(2) * attn

    @pl.when(step < last_step)
    def _():
        for copy in send_fresh(layer, own):
            copy.start()

    @pl.when(step == last_step)
    def _():
        for copy in send_final(layer, own) + keep_final(layer, own):
            copy.start()

    h2 = (normed(r) * (1.0 + mod(4)) + mod(3)).astype(BF16)
    chunk = 512
    down = None
    for base in range(0, up_ref.shape[2], chunk):
        up = jnp.dot(h2, up_ref[0, :, base:base + chunk], preferred_element_type=F32)
        act = gelu(up).astype(BF16)
        term = jnp.dot(act, down_ref[0, base:base + chunk, :], preferred_element_type=F32)
        down = term if down is None else down + term
    r = r + mod(5) * down
    resid[...] = r

    @pl.when(layer == n_layers - 1)
    def _():
        eps = jnp.dot(normed(resid[...]).astype(BF16), head_ref[...], preferred_element_type=F32)

        @pl.when(step > 0)
        def _():
            send_eps().wait_send()

        eps_send[...] = eps.astype(BF16)
        send_eps().start()
        send_eps().wait_recv()
        mine = eps_send[...].astype(F32)
        peer = eps_recv[step].astype(F32)
        is_cond = slot % 2 == 0
        eps_cond = jnp.where(is_cond, mine, peer)
        eps_unc = jnp.where(is_cond, peer, mine)
        guided = eps_unc + sched_ref[2, step] * (eps_cond - eps_unc)
        x_out[0] = sched_ref[0, step] * x_out[0] + sched_ref[1, step] * guided

    @pl.when((step == last_step) & (layer == n_layers - 1))
    def _():
        send_eps().wait_send()
        for at_layer in (n_layers - 2, n_layers - 1):
            at_slot = (last_step * n_layers + at_layer) % 2
            for copy in send_final(at_layer, at_slot):
                copy.wait_send()
            for copy in keep_final(at_layer, at_slot):
                copy.wait()
        for at_layer in range(n_layers):
            for copy in send_final(at_layer, at_layer % 2):
                copy.wait_recv()


def solution(mesh):
    slot_spec = P(("img", "cfg"), None, None)
    cache_spec = P(("img", "cfg"), None, None, None)
    rep_spec = P()

    def local_step(latent, cond_vec, sched_coef, w_ada, w_qkv, w_out, w_up, w_down, w_head, k_stale, v_stale):
        n_layers, width = w_qkv.shape[0], w_qkv.shape[1]
        rows = latent.shape[1]
        n_heads, head_dim = w_out.shape[1], w_out.shape[2]
        n_steps = sched_coef.shape[1]
        w_out = w_out.reshape(n_layers, width, width)

        def per_layer(array):
            return pl.BlockSpec((1,) + array.shape[1:], lambda s, l: (l, 0, 0))

        any_spec = pl.BlockSpec(memory_space=pl.ANY)
        vmem_spec = pl.BlockSpec(memory_space=pltpu.VMEM)
        x_new, k_new, v_new = pl.pallas_call(
            functools.partial(kernel, n_steps, n_layers, n_heads, head_dim),
            grid=(n_steps, n_layers),
            out_shape=[
                jax.ShapeDtypeStruct((1, rows, width), F32),
                jax.ShapeDtypeStruct(k_stale.shape, BF16),
                jax.ShapeDtypeStruct(v_stale.shape, BF16),
            ],
            in_specs=[
                any_spec,
                vmem_spec,
                pl.BlockSpec(memory_space=pltpu.SMEM),
                pl.BlockSpec((1,) + w_ada.shape[1:], lambda s, l: (jnp.where(s == 0, l, n_layers - 1), 0, 0)),
                per_layer(w_qkv),
                per_layer(w_out),
                per_layer(w_up),
                per_layer(w_down),
                vmem_spec,
                any_spec,
                any_spec,
            ],
            out_specs=[vmem_spec, any_spec, any_spec],
            scratch_shapes=[
                pltpu.VMEM((rows, width), BF16),
                pltpu.VMEM((rows, width), F32),
                pltpu.VMEM((n_layers, 8, 6 * width), F32),
                pltpu.VMEM((width, rows), BF16),
                pltpu.VMEM((2, 2, rows, width), BF16),
                pltpu.VMEM((n_layers + 2, 2, rows, width), BF16),
                pltpu.VMEM((rows, width), BF16),
                pltpu.VMEM((n_steps, rows, width), BF16),
                pltpu.SemaphoreType.DMA,
                pltpu.SemaphoreType.DMA((2, 2)),
                pltpu.SemaphoreType.DMA((2, 2)),
                pltpu.SemaphoreType.DMA((n_layers, 2)),
                pltpu.SemaphoreType.DMA((n_layers, 2)),
                pltpu.SemaphoreType.DMA((2, 2)),
                pltpu.SemaphoreType.DMA,
                pltpu.SemaphoreType.DMA((n_steps,)),
            ],
            compiler_params=pltpu.CompilerParams(
                collective_id=0, has_side_effects=True, vmem_limit_bytes=48 * 1024 * 1024,
                dimension_semantics=("arbitrary", "arbitrary"),
            ),
            name="denoise",
        )(latent, cond_vec, sched_coef, w_ada, w_qkv, w_out, w_up, w_down, w_head, k_stale, v_stale)
        return x_new, k_new, v_new

    return jax.shard_map(
        local_step,
        mesh=mesh,
        in_specs=(P("img", "patch", None), slot_spec, rep_spec, rep_spec, rep_spec, rep_spec, rep_spec, rep_spec, rep_spec, cache_spec, cache_spec),
        out_specs=(P(("img", "cfg"), "patch", None), cache_spec, cache_spec),
        check_vma=False,
    )
```

```python
import functools
import math

import jax
import jax.numpy as jnp
from jax import lax
from jax.experimental import pallas as pl
from jax.experimental.pallas import tpu as pltpu
from jax.sharding import PartitionSpec as P

MESH = pl.DeviceIdType.MESH
F32 = jnp.float32
BF16 = jnp.bfloat16
VMEM_ALL = 67043328
GELU_A = math.sqrt(2.0 / math.pi)
GELU_B = GELU_A * 0.044715


def normed(values):
    row_mean = jnp.mean(values, -1, keepdims=True)
    centered = values - row_mean
    row_var = jnp.mean(centered * centered, -1, keepdims=True)
    return centered * lax.rsqrt(row_var + 1e-6)


def gelu(x):
    half = 0.5 * x
    return half + half * jnp.tanh(x * (GELU_A + GELU_B * (x * x)))


def contract(a, b, a_dim, b_dim):
    return lax.dot_general(a, b, (((a_dim,), (b_dim,)), ((), ())), preferred_element_type=F32)


def kernel(
    n_steps, n_layers, n_heads, head_dim,
    latent_hbm, cond_ref, sched_ref, ada_ref, qkv_ref, out_ref, up_ref, down_ref, head_ref, k_stale, v_stale,
    x_out, eps_out, kv_fin,
    lat_buf, resid, mod_buf, o_buf, s_buf, p_buf, kv_own, kv_peer, eps_recv,
    lat_sem, stale_sem, send_sem, recv_sem, last_sem, keep_sem, eps_send_sem, eps_recv_sem,
):
    step = pl.program_id(0)
    layer = pl.program_id(1)
    rows, width = resid.shape
    patch = lax.axis_index("patch")
    slot = lax.axis_index("cfg")
    other = 1 - patch
    partner = slot + 1 - 2 * (slot % 2)
    peer_rows = pl.ds(pl.multiple_of(other * rows, rows), rows)
    last_step = n_steps - 1
    first = (step == 0) & (layer == 0)

    def load_stale(at_layer):
        place = n_layers + at_layer % 2
        return [
            pltpu.make_async_copy(src.at[0, at_layer, peer_rows], kv_peer.at[place, part], stale_sem.at[at_layer % 2, part])
            for part, src in enumerate((k_stale, v_stale))
        ]

    def send_kv(at_layer, target, arrival):
        return [
            pltpu.make_async_remote_copy(
                src_ref=kv_own.at[at_layer, part], dst_ref=target.at[at_layer, part],
                send_sem=send_sem.at[at_layer, part], recv_sem=arrival.at[at_layer, part],
                device_id={"patch": other}, device_id_type=MESH)
            for part in range(2)
        ]

    def send_fresh(at_layer):
        return send_kv(at_layer, kv_peer, recv_sem)

    def send_final(at_layer):
        return send_kv(at_layer, kv_fin.at[1], last_sem)

    def keep_final(at_layer):
        return [
            pltpu.make_async_copy(kv_own.at[at_layer, part], kv_fin.at[0, at_layer, part], keep_sem.at[at_layer, part])
            for part in range(2)
        ]

    def send_eps():
        return pltpu.make_async_remote_copy(
            src_ref=eps_out, dst_ref=eps_recv.at[step],
            send_sem=eps_send_sem, recv_sem=eps_recv_sem.at[step],
            device_id={"cfg": partner}, device_id_type=MESH)

    @pl.when(first)
    def _():
        barrier = pltpu.get_barrier_semaphore()
        pl.semaphore_signal(barrier, inc=1, device_id={"patch": other}, device_id_type=MESH)
        pl.semaphore_signal(barrier, inc=1, device_id={"cfg": partner}, device_id_type=MESH)
        fetch = pltpu.make_async_copy(latent_hbm.at[slot // 2], lat_buf, lat_sem)
        fetch.start()
        for copy in load_stale(0):
            copy.start()
        fetch.wait()
        x_out[...] = lat_buf[...].astype(F32)
        pl.semaphore_wait(barrier, 2)

    @pl.when(step == 0)
    def _():
        cond = cond_ref[0]
        act = (cond * jax.nn.sigmoid(cond)).astype(BF16)
        mod_buf[layer, 0:n_steps, :] = jnp.dot(act, ada_ref[0], preferred_element_type=F32)

        for copy in load_stale(layer):
            copy.wait()

        @pl.when(layer + 1 < n_layers)
        def _():
            for copy in load_stale(layer + 1):
                copy.start()

    @pl.when(step > 0)
    def _():
        for copy in send_fresh(layer):
            copy.wait_recv()
            copy.wait_send()

    @pl.when(layer == 0)
    def _():
        resid[...] = x_out[...]

    def mod(part):
        return mod_buf[layer, pl.ds(step, 1), part * width:(part + 1) * width]

    h = (normed(resid[...]) * (1.0 + mod(1)) + mod(0)).astype(BF16)
    qkv = jnp.dot(h, qkv_ref[0], preferred_element_type=F32).astype(BF16)

    kv_own[layer, 0] = qkv[:, width:2 * width]
    kv_own[layer, 1] = qkv[:, 2 * width:]

    place = jnp.where(step == 0, n_layers + layer % 2, layer)
    factor = head_dim ** -0.5 * math.log2(math.e)
    pair_width = 2 * head_dim
    lane = lax.broadcasted_iota(jnp.int32, (rows, pair_width), 1)
    tops, totals = {}, {}

    def cols_of(head):
        base = head // 2 * pair_width
        return slice(base, base + pair_width)

    def score(head):
        cols = cols_of(head)
        keep = (lane < head_dim) if head % 2 == 0 else (lane >= head_dim)
        q_head = jnp.where(keep, qkv[:, cols], jnp.zeros((rows, pair_width), BF16))
        top = None
        for side, keys in enumerate((kv_own[layer, 0, :, cols], kv_peer[place, 0, :, cols])):
            s = contract(keys, q_head, 1, 1)
            s_buf[head % 2, side] = s
            side_top = jnp.max(s, 0, keepdims=True)
            top = side_top if top is None else jnp.maximum(top, side_top)
        tops[head] = top

    def weigh(head):
        total = None
        for side in range(2):
            e = jnp.exp2((s_buf[head % 2, side] - tops[head]) * factor)
            p_buf[head % 2, side] = e.astype(BF16)
            side_total = jnp.sum(e, 0, keepdims=True)
            total = side_total if total is None else total + side_total
        totals[head] = total

    def mix(head):
        cols = cols_of(head)
        part = slice(head % 2 * head_dim, (head % 2 + 1) * head_dim)
        mixed = None
        for side, values in enumerate((kv_own[layer, 1, :, cols], kv_peer[place, 1, :, cols])):
            term = contract(values.T[part], p_buf[head % 2, side], 1, 0)
            mixed = term if mixed is None else mixed + term
        o_buf[head * head_dim:(head + 1) * head_dim, :] = (mixed * (1.0 / totals[head])).astype(BF16)

    for turn in range(n_heads + 2):
        if turn < n_heads:
            score(turn)
        if 1 <= turn <= n_heads:
            weigh(turn - 1)
        if turn >= 2:
            mix(turn - 2)

    attn = contract(o_buf[...], out_ref[0], 0, 0)
    r = resid[...] + mod(2) * attn

    h2 = (normed(r) * (1.0 + mod(4)) + mod(3)).astype(BF16)
    chunk = 512
    down = None
    for base in range(0, up_ref.shape[2], chunk):
        up = jnp.dot(h2, up_ref[0, :, base:base + chunk], preferred_element_type=F32)
        act = gelu(up).astype(BF16)
        term = jnp.dot(act, down_ref[0, base:base + chunk, :], preferred_element_type=F32)
        down = term if down is None else down + term
    r = r + mod(5) * down
    resid[...] = r

    @pl.when(step < last_step)
    def _():
        for copy in send_fresh(layer):
            copy.start()

    @pl.when(step == last_step)
    def _():
        for copy in send_final(layer) + keep_final(layer):
            copy.start()

    @pl.when(layer == n_layers - 1)
    def _():
        @pl.when((step > 0) & (step < n_steps))
        def _():
            send_eps().wait_send()

        eps = jnp.dot(normed(resid[...]).astype(BF16), head_ref[...], preferred_element_type=F32)
        eps_out[...] = eps.astype(BF16)

    @pl.when((step < last_step) & (layer == n_layers - 1))
    def _():
        send_eps().start()
        send_eps().wait_recv()
        x_out[...] = guide(slot, sched_ref, step, x_out[...], eps_out[...], eps_recv[step])

    @pl.when((step == last_step) & (layer == n_layers - 1))
    def _():
        for at_layer in range(n_layers):
            for copy in send_final(at_layer):
                copy.wait_send()
                copy.wait_recv()
            for copy in keep_final(at_layer):
                copy.wait()


def guide(slot, sched, step, x, mine, peer):
    mine, peer = mine.astype(F32), peer.astype(F32)
    is_cond = slot % 2 == 0
    eps_cond = jnp.where(is_cond, mine, peer)
    eps_unc = jnp.where(is_cond, peer, mine)
    guided = eps_unc + sched[step, 2] * (eps_cond - eps_unc)
    return sched[step, 0] * x + sched[step, 1] * guided


def store_kernel(kv_fin, k_out, v_out, buf, in_sem, out_sem):
    n_layers, rows = buf.shape[1], buf.shape[3]
    patch = lax.axis_index("patch")
    loads, stores = [], []
    for layer in range(n_layers):
        for side, owner in enumerate((patch, 1 - patch)):
            for part, dst in enumerate((k_out, v_out)):
                at = pl.ds(pl.multiple_of(owner * rows, rows), rows)
                here = buf.at[side, layer, part]
                loads.append(pltpu.make_async_copy(kv_fin.at[side, layer, part], here, in_sem.at[side, layer, part]))
                stores.append(pltpu.make_async_copy(here, dst.at[0, layer, at], out_sem.at[side, layer, part]))
    for copy in loads:
        copy.start()
    for load, store in zip(loads, stores):
        load.wait()
        store.start()
    for copy in stores:
        copy.wait()


def solution(mesh):
    slot_spec = P(("img", "cfg"), None, None)
    cache_spec = P(("img", "cfg"), None, None, None)
    rep_spec = P()
    n_cfg = mesh.shape["cfg"]
    partner = [(at, at ^ 1) for at in range(n_cfg)]

    def local_step(latent, cond_vec, sched_coef, w_ada, w_qkv, w_out, w_up, w_down, w_head, k_stale, v_stale):
        n_layers, width = w_qkv.shape[0], w_qkv.shape[1]
        rows = latent.shape[1]
        n_heads, head_dim = w_out.shape[1], w_out.shape[2]
        n_steps = sched_coef.shape[1]
        w_out = w_out.reshape(n_layers, width, width)

        def per_layer(array):
            return pl.BlockSpec((1,) + array.shape[1:], lambda s, l: (l, 0, 0))

        def whole(array):
            return pl.BlockSpec(array.shape, lambda s, l: (0,) * array.ndim)

        any_spec = pl.BlockSpec(memory_space=pl.ANY)
        vmem_spec = pl.BlockSpec(memory_space=pltpu.VMEM)
        kv_shape = (2, n_layers, 2, rows, width)
        x_last, eps, kv_fin = pl.pallas_call(
            functools.partial(kernel, n_steps, n_layers, n_heads, head_dim),
            grid=(n_steps, n_layers),
            out_shape=[
                jax.ShapeDtypeStruct((rows, width), F32),
                jax.ShapeDtypeStruct((rows, width), BF16),
                jax.ShapeDtypeStruct(kv_shape, BF16),
            ],
            in_specs=[
                any_spec,
                whole(cond_vec),
                pl.BlockSpec(memory_space=pltpu.SMEM),
                pl.BlockSpec((1,) + w_ada.shape[1:], lambda s, l: (jnp.where(s == 0, l, n_layers - 1), 0, 0)),
                per_layer(w_qkv),
                per_layer(w_out),
                per_layer(w_up),
                per_layer(w_down),
                whole(w_head),
                any_spec,
                any_spec,
            ],
            out_specs=[vmem_spec, vmem_spec, any_spec],
            scratch_shapes=[
                pltpu.VMEM((rows, width), BF16),
                pltpu.VMEM((rows, width), F32),
                pltpu.VMEM((n_layers, 8, 6 * width), F32),
                pltpu.VMEM((width, rows), BF16),
                pltpu.VMEM((2, 2, rows, rows), F32),
                pltpu.VMEM((2, 2, rows, rows), BF16),
                pltpu.VMEM((n_layers, 2, rows, width), BF16),
                pltpu.VMEM((n_layers + 2, 2, rows, width), BF16),
                pltpu.VMEM((n_steps, rows, width), BF16),
                pltpu.SemaphoreType.DMA,
                pltpu.SemaphoreType.DMA((2, 2)),
                pltpu.SemaphoreType.DMA((n_layers, 2)),
                pltpu.SemaphoreType.DMA((n_layers, 2)),
                pltpu.SemaphoreType.DMA((n_layers, 2)),
                pltpu.SemaphoreType.DMA((n_layers, 2)),
                pltpu.SemaphoreType.DMA,
                pltpu.SemaphoreType.DMA((n_steps,)),
            ],
            compiler_params=pltpu.CompilerParams(
                collective_id=0, has_side_effects=True, vmem_limit_bytes=VMEM_ALL,
                dimension_semantics=("arbitrary", "arbitrary"),
            ),
            name="denoise",
        )(latent, cond_vec, sched_coef.T, w_ada, w_qkv, w_out, w_up, w_down, w_head, k_stale, v_stale)
        eps_peer = lax.ppermute(eps, "cfg", partner)
        k_new, v_new = pl.pallas_call(
            store_kernel,
            out_shape=[jax.ShapeDtypeStruct(k_stale.shape, BF16), jax.ShapeDtypeStruct(v_stale.shape, BF16)],
            in_specs=[any_spec],
            out_specs=[any_spec] * 2,
            scratch_shapes=[
                pltpu.VMEM(kv_shape, BF16),
                pltpu.SemaphoreType.DMA(kv_shape[:3]),
                pltpu.SemaphoreType.DMA(kv_shape[:3]),
            ],
            compiler_params=pltpu.CompilerParams(vmem_limit_bytes=VMEM_ALL),
            cost_estimate=pl.CostEstimate(flops=0, bytes_accessed=2 * 2 * k_stale.size * 2, transcendentals=0),
            name="store",
        )(kv_fin)
        x_new = guide(lax.axis_index("cfg"), sched_coef.T, n_steps - 1, x_last, eps, eps_peer)
        return x_new[None], k_new, v_new

    return jax.shard_map(
        local_step,
        mesh=mesh,
        in_specs=(P("img", "patch", None), slot_spec, rep_spec, rep_spec, rep_spec, rep_spec, rep_spec, rep_spec, rep_spec, cache_spec, cache_spec),
        out_specs=(P(("img", "cfg"), "patch", None), cache_spec, cache_spec),
        check_vma=False,
    )
```

```python
import functools
import math

import jax
import jax.numpy as jnp
from jax import lax
from jax.experimental import pallas as pl
from jax.experimental.pallas import tpu as pltpu
from jax.sharding import PartitionSpec as P

MESH = pl.DeviceIdType.MESH
F32 = jnp.float32
BF16 = jnp.bfloat16
VMEM_ALL = 67043328
GELU_A = math.sqrt(2.0 / math.pi)
GELU_B = GELU_A * 0.044715


def normed(values):
    row_mean = jnp.mean(values, -1, keepdims=True)
    centered = values - row_mean
    row_var = jnp.mean(centered * centered, -1, keepdims=True)
    return centered * lax.rsqrt(row_var + 1e-6)


def gelu_of_half(half):
    return half + half * jnp.tanh(half * (2.0 * GELU_A + 8.0 * GELU_B * (half * half)))


def contract(a, b, a_dim, b_dim):
    return lax.dot_general(a, b, (((a_dim,), (b_dim,)), ((), ())), preferred_element_type=F32)


def kernel(
    n_steps, n_layers, n_heads, head_dim,
    latent_hbm, cond_hbm, sched_hbm, ada_hbm, qkv_hbm, out_hbm, up_hbm, down_hbm, head_hbm, k_stale, v_stale,
    x_out, eps_out, kv_fin,
    sched_ref, cond_buf, lat_buf, head_buf, ada_buf, qkv_buf, out_buf, up_buf, down_buf,
    resid, mod_buf, o_buf, s_buf, p_buf, kv_own, kv_peer, eps_recv,
    small_sem, ada_sem, weight_sem, stale_sem, send_sem, recv_sem, last_sem, keep_sem, eps_send_sem, eps_recv_sem,
):
    rows, width = resid.shape
    patch = lax.axis_index("patch")
    slot = lax.axis_index("cfg")
    other = 1 - patch
    partner = slot + 1 - 2 * (slot % 2)
    peer_rows = pl.ds(pl.multiple_of(other * rows, rows), rows)
    last_step = n_steps - 1

    def start(copies):
        for copy in copies:
            copy.start()

    def wait(copies):
        for copy in copies:
            copy.wait()

    def load_small():
        pairs = ((latent_hbm.at[slot // 2], lat_buf), (cond_hbm.at[0], cond_buf), (sched_hbm, sched_ref), (head_hbm, head_buf))
        return [pltpu.make_async_copy(src, dst, small_sem.at[at]) for at, (src, dst) in enumerate(pairs)]

    def load_ada(at_layer):
        return [pltpu.make_async_copy(ada_hbm.at[at_layer], ada_buf.at[at_layer % 2], ada_sem.at[at_layer % 2])]

    def load_weights(at_layer):
        pairs = ((qkv_hbm, qkv_buf), (out_hbm, out_buf), (up_hbm, up_buf), (down_hbm, down_buf))
        return [
            pltpu.make_async_copy(src.at[at_layer], dst.at[at_layer % 2], weight_sem.at[at_layer % 2, at])
            for at, (src, dst) in enumerate(pairs)
        ]

    def load_stale(at_layer):
        place = n_layers + at_layer % 2
        return [
            pltpu.make_async_copy(src.at[0, at_layer, peer_rows], kv_peer.at[place, part], stale_sem.at[at_layer % 2, part])
            for part, src in enumerate((k_stale, v_stale))
        ]

    def send_kv(at_layer, target, arrival):
        return [
            pltpu.make_async_remote_copy(
                src_ref=kv_own.at[at_layer, part], dst_ref=target.at[at_layer, part],
                send_sem=send_sem.at[at_layer, part], recv_sem=arrival.at[at_layer, part],
                device_id={"patch": other}, device_id_type=MESH)
            for part in range(2)
        ]

    def send_fresh(at_layer):
        return send_kv(at_layer, kv_peer, recv_sem)

    def send_final(at_layer):
        return send_kv(at_layer, kv_fin.at[1], last_sem)

    def keep_final(at_layer):
        return [
            pltpu.make_async_copy(kv_own.at[at_layer, part], kv_fin.at[0, at_layer, part], keep_sem.at[at_layer, part])
            for part in range(2)
        ]

    def send_eps(at_step):
        return pltpu.make_async_remote_copy(
            src_ref=eps_out, dst_ref=eps_recv.at[at_step],
            send_sem=eps_send_sem, recv_sem=eps_recv_sem.at[at_step],
            device_id={"cfg": partner}, device_id_type=MESH)

    def modulate(at_layer):
        cond = cond_buf[...]
        act = (cond * jax.nn.sigmoid(cond)).astype(BF16)
        mod_buf[at_layer, 0:n_steps, :] = jnp.dot(act, ada_buf[at_layer % 2], preferred_element_type=F32)

    def block(step, layer):
        side = layer % 2
        wait(load_weights(layer))
        if step == 0:
            wait(load_stale(layer))

            @pl.when(layer + 1 < n_layers)
            def _():
                wait(load_ada(layer + 1))
                start(load_stale(layer + 1))

            @pl.when(layer + 2 < n_layers)
            def _():
                start(load_ada(layer + 2))
        else:
            for copy in send_fresh(layer):
                copy.wait_recv()
                copy.wait_send()
        if step < last_step:
            start(load_weights(lax.rem(layer + 1, n_layers)))
        else:
            @pl.when(layer + 1 < n_layers)
            def _():
                start(load_weights(layer + 1))

        def mod(part):
            return mod_buf[layer, step:step + 1, part * width:(part + 1) * width]

        h = (normed(resid[...]) * (1.0 + mod(1)) + mod(0)).astype(BF16)
        qkv = jnp.dot(h, qkv_buf[side], preferred_element_type=F32).astype(BF16)
        kv_own[layer, 0] = qkv[:, width:2 * width]
        kv_own[layer, 1] = qkv[:, 2 * width:]

        place = n_layers + layer % 2 if step == 0 else layer
        factor = head_dim ** -0.5 * math.log2(math.e)
        pair_width = 2 * head_dim
        lane = lax.broadcasted_iota(jnp.int32, (rows, pair_width), 1)
        tops, totals = {}, {}

        def cols_of(head):
            base = head // 2 * pair_width
            return slice(base, base + pair_width)

        def score(head):
            cols = cols_of(head)
            keep = (lane < head_dim) if head % 2 == 0 else (lane >= head_dim)
            q_head = jnp.where(keep, qkv[:, cols], jnp.zeros((rows, pair_width), BF16))
            top = None
            for side, keys in enumerate((kv_own[layer, 0, :, cols], kv_peer[place, 0, :, cols])):
                s = contract(keys, q_head, 1, 1)
                s_buf[head % 2, side] = s
                side_top = jnp.max(s, 0, keepdims=True)
                top = side_top if top is None else jnp.maximum(top, side_top)
            tops[head] = top

        def weigh(head):
            total = None
            for side in range(2):
                e = jnp.exp2((s_buf[head % 2, side] - tops[head]) * factor)
                p_buf[head % 2, side] = e.astype(BF16)
                side_total = jnp.sum(e, 0, keepdims=True)
                total = side_total if total is None else total + side_total
            totals[head] = total

        def mix(head):
            cols = cols_of(head)
            part = slice(head % 2 * head_dim, (head % 2 + 1) * head_dim)
            mixed = None
            for side, values in enumerate((kv_own[layer, 1, :, cols], kv_peer[place, 1, :, cols])):
                term = contract(values.T[part], p_buf[head % 2, side], 1, 0)
                mixed = term if mixed is None else mixed + term
            o_buf[head * head_dim:(head + 1) * head_dim, :] = (mixed * (1.0 / totals[head])).astype(BF16)

        for turn in range(n_heads + 2):
            if turn < n_heads:
                score(turn)
            if 1 <= turn <= n_heads:
                weigh(turn - 1)
            if turn >= 2:
                mix(turn - 2)

        if step == 0:
            modulate(layer + 1)

        attn = contract(o_buf[...], out_buf[side], 0, 0)
        r = resid[...] + mod(2) * attn
        h2 = (normed(r) * (0.5 * (1.0 + mod(4))) + 0.5 * mod(3)).astype(BF16)
        chunk = 512
        down = None
        for base in range(0, up_buf.shape[2], chunk):
            half = jnp.dot(h2, up_buf[side, :, base:base + chunk], preferred_element_type=F32)
            act = gelu_of_half(half).astype(BF16)
            term = jnp.dot(act, down_buf[side, base:base + chunk, :], preferred_element_type=F32)
            down = term if down is None else down + term
        resid[...] = r + mod(5) * down
        if step < last_step:
            start(send_fresh(layer))
        else:
            start(send_final(layer) + keep_final(layer))

    barrier = pltpu.get_barrier_semaphore()
    pl.semaphore_signal(barrier, inc=1, device_id={"patch": other}, device_id_type=MESH)
    pl.semaphore_signal(barrier, inc=1, device_id={"cfg": partner}, device_id_type=MESH)
    start(load_small())
    start(load_ada(0))
    start(load_weights(0))
    start(load_stale(0))
    start(load_ada(1))
    wait(load_small())
    x_out[...] = lat_buf[...].astype(F32)
    resid[...] = lat_buf[...].astype(F32)
    wait(load_ada(0))
    modulate(0)
    pl.semaphore_wait(barrier, 2)

    for step in range(n_steps):
        lax.fori_loop(0, n_layers, lambda layer, carry: (block(step, layer), carry)[1], 0)
        if step > 0:
            send_eps(step - 1).wait_send()
        eps = jnp.dot(normed(resid[...]).astype(BF16), head_buf[...], preferred_element_type=F32)
        eps_out[...] = eps.astype(BF16)
        if step < last_step:
            send_eps(step).start()
            send_eps(step).wait_recv()
            x_now = guide(slot, sched_ref, step, x_out[...], eps_out[...], eps_recv[step])
            x_out[...] = x_now
            resid[...] = x_now

    def drain(at_layer, carry):
        for copy in send_final(at_layer):
            copy.wait_send()
            copy.wait_recv()
        wait(keep_final(at_layer))
        return carry

    lax.fori_loop(0, n_layers, drain, 0)


def guide(slot, sched, step, x, mine, peer):
    mine, peer = mine.astype(F32), peer.astype(F32)
    is_cond = slot % 2 == 0
    eps_cond = jnp.where(is_cond, mine, peer)
    eps_unc = jnp.where(is_cond, peer, mine)
    guided = eps_unc + sched[step, 2] * (eps_cond - eps_unc)
    return sched[step, 0] * x + sched[step, 1] * guided


def store_kernel(kv_fin, k_out, v_out, buf, in_sem, out_sem):
    n_layers, rows = buf.shape[1], buf.shape[3]
    patch = lax.axis_index("patch")
    loads, stores = [], []
    for layer in range(n_layers):
        for side, owner in enumerate((patch, 1 - patch)):
            for part, dst in enumerate((k_out, v_out)):
                at = pl.ds(pl.multiple_of(owner * rows, rows), rows)
                here = buf.at[side, layer, part]
                loads.append(pltpu.make_async_copy(kv_fin.at[side, layer, part], here, in_sem.at[side, layer, part]))
                stores.append(pltpu.make_async_copy(here, dst.at[0, layer, at], out_sem.at[side, layer, part]))
    for copy in loads:
        copy.start()
    for load, store in zip(loads, stores):
        load.wait()
        store.start()
    for copy in stores:
        copy.wait()


def guide_kernel(step, sched_ref, x_ref, mine_ref, peer_ref, x_new):
    x_new[0] = guide(lax.axis_index("cfg"), sched_ref, step, x_ref[...], mine_ref[...], peer_ref[...])


def solution(mesh):
    slot_spec = P(("img", "cfg"), None, None)
    cache_spec = P(("img", "cfg"), None, None, None)
    rep_spec = P()
    n_cfg = mesh.shape["cfg"]
    partner = [(at, at ^ 1) for at in range(n_cfg)]

    def local_step(latent, cond_vec, sched_coef, w_ada, w_qkv, w_out, w_up, w_down, w_head, k_stale, v_stale):
        n_layers, width = w_qkv.shape[0], w_qkv.shape[1]
        rows = latent.shape[1]
        n_heads, head_dim = w_out.shape[1], w_out.shape[2]
        n_steps = sched_coef.shape[1]
        w_out = w_out.reshape(n_layers, width, width)

        any_spec = pl.BlockSpec(memory_space=pl.ANY)
        vmem_spec = pl.BlockSpec(memory_space=pltpu.VMEM)
        kv_shape = (2, n_layers, 2, rows, width)
        x_last, eps, kv_fin = pl.pallas_call(
            functools.partial(kernel, n_steps, n_layers, n_heads, head_dim),
            out_shape=[
                jax.ShapeDtypeStruct((rows, width), F32),
                jax.ShapeDtypeStruct((rows, width), BF16),
                jax.ShapeDtypeStruct(kv_shape, BF16),
            ],
            in_specs=[any_spec] * 11,
            out_specs=[vmem_spec, vmem_spec, any_spec],
            scratch_shapes=[
                pltpu.SMEM(sched_coef.shape[::-1], F32),
                pltpu.VMEM(cond_vec.shape[1:], F32),
                pltpu.VMEM((rows, width), BF16),
                pltpu.VMEM(w_head.shape, BF16),
                pltpu.VMEM((2,) + w_ada.shape[1:], BF16),
                pltpu.VMEM((2,) + w_qkv.shape[1:], BF16),
                pltpu.VMEM((2,) + w_out.shape[1:], BF16),
                pltpu.VMEM((2,) + w_up.shape[1:], BF16),
                pltpu.VMEM((2,) + w_down.shape[1:], BF16),
                pltpu.VMEM((rows, width), F32),
                pltpu.VMEM((n_layers + 1, 8, 6 * width), F32),
                pltpu.VMEM((width, rows), BF16),
                pltpu.VMEM((2, 2, rows, rows), F32),
                pltpu.VMEM((2, 2, rows, rows), BF16),
                pltpu.VMEM((n_layers, 2, rows, width), BF16),
                pltpu.VMEM((n_layers + 2, 2, rows, width), BF16),
                pltpu.VMEM((n_steps, rows, width), BF16),
                pltpu.SemaphoreType.DMA((4,)),
                pltpu.SemaphoreType.DMA((2,)),
                pltpu.SemaphoreType.DMA((2, 4)),
                pltpu.SemaphoreType.DMA((2, 2)),
                pltpu.SemaphoreType.DMA((n_layers, 2)),
                pltpu.SemaphoreType.DMA((n_layers, 2)),
                pltpu.SemaphoreType.DMA((n_layers, 2)),
                pltpu.SemaphoreType.DMA((n_layers, 2)),
                pltpu.SemaphoreType.DMA,
                pltpu.SemaphoreType.DMA((n_steps,)),
            ],
            compiler_params=pltpu.CompilerParams(
                collective_id=0, has_side_effects=True, vmem_limit_bytes=VMEM_ALL,
            ),
            name="denoise",
        )(latent, cond_vec, sched_coef.T, w_ada, w_qkv, w_out, w_up, w_down, w_head, k_stale, v_stale)
        eps_peer = lax.ppermute(eps, "cfg", partner)
        k_new, v_new = pl.pallas_call(
            store_kernel,
            out_shape=[jax.ShapeDtypeStruct(k_stale.shape, BF16), jax.ShapeDtypeStruct(v_stale.shape, BF16)],
            in_specs=[any_spec],
            out_specs=[any_spec] * 2,
            scratch_shapes=[
                pltpu.VMEM(kv_shape, BF16),
                pltpu.SemaphoreType.DMA(kv_shape[:3]),
                pltpu.SemaphoreType.DMA(kv_shape[:3]),
            ],
            compiler_params=pltpu.CompilerParams(vmem_limit_bytes=VMEM_ALL),
            cost_estimate=pl.CostEstimate(flops=0, bytes_accessed=2 * 2 * k_stale.size * 2, transcendentals=0),
            name="store",
        )(kv_fin)
        x_new = pl.pallas_call(
            functools.partial(guide_kernel, n_steps - 1),
            out_shape=jax.ShapeDtypeStruct((1, rows, width), F32),
            in_specs=[pl.BlockSpec(memory_space=pltpu.SMEM)] + [vmem_spec] * 3,
            out_specs=vmem_spec,
            name="guide",
        )(sched_coef.T, x_last, eps, eps_peer)
        return x_new, k_new, v_new

    return jax.shard_map(
        local_step,
        mesh=mesh,
        in_specs=(P("img", "patch", None), slot_spec, rep_spec, rep_spec, rep_spec, rep_spec, rep_spec, rep_spec, rep_spec, cache_spec, cache_spec),
        out_specs=(P(("img", "cfg"), "patch", None), cache_spec, cache_spec),
        check_vma=False,
    )
```

```python
import functools
import math

import jax
import jax.numpy as jnp
from jax import lax
from jax.experimental import pallas as pl
from jax.experimental.pallas import tpu as pltpu
from jax.sharding import PartitionSpec as P

MESH = pl.DeviceIdType.MESH
F32 = jnp.float32
BF16 = jnp.bfloat16
VMEM_ALL = 67043328
GELU_A = math.sqrt(2.0 / math.pi)
GELU_B = GELU_A * 0.044715


def normed(values):
    row_mean = jnp.mean(values, -1, keepdims=True)
    centered = values - row_mean
    row_var = jnp.mean(centered * centered, -1, keepdims=True)
    return centered * lax.rsqrt(row_var + 1e-6)


def gelu_of_half(half):
    return half + half * jnp.tanh(half * (2.0 * GELU_A + 8.0 * GELU_B * (half * half)))


def contract(a, b, a_dim, b_dim):
    return lax.dot_general(a, b, (((a_dim,), (b_dim,)), ((), ())), preferred_element_type=F32)


def kernel(
    n_steps, n_layers, n_heads, head_dim,
    latent_hbm, cond_hbm, sched_hbm, ada_hbm, qkv_hbm, out_hbm, up_hbm, down_hbm, head_hbm, k_stale, v_stale,
    x_out, eps_out, kv_fin,
    sched_ref, cond_buf, lat_buf, head_buf, ada_buf, qkv_buf, out_buf, up_buf, down_buf,
    resid, mod_buf, o_buf, s_buf, p_buf, kv_own, kv_peer, eps_recv,
    small_sem, ada_sem, weight_sem, stale_sem, send_sem, recv_sem, last_sem, keep_sem, eps_send_sem, eps_recv_sem,
):
    rows, width = resid.shape
    patch = lax.axis_index("patch")
    slot = lax.axis_index("cfg")
    other = 1 - patch
    partner = slot + 1 - 2 * (slot % 2)
    peer_rows = pl.ds(pl.multiple_of(other * rows, rows), rows)
    last_step = n_steps - 1

    def start(copies):
        for copy in copies:
            copy.start()

    def wait(copies):
        for copy in copies:
            copy.wait()

    def load_small():
        pairs = ((latent_hbm.at[slot // 2], lat_buf), (cond_hbm.at[0], cond_buf), (sched_hbm, sched_ref), (head_hbm, head_buf))
        return [pltpu.make_async_copy(src, dst, small_sem.at[at]) for at, (src, dst) in enumerate(pairs)]

    def load_ada(at_layer):
        return [pltpu.make_async_copy(ada_hbm.at[at_layer], ada_buf.at[at_layer % 2], ada_sem.at[at_layer % 2])]

    def load_weights(at_layer):
        pairs = ((qkv_hbm, qkv_buf), (out_hbm, out_buf), (up_hbm, up_buf), (down_hbm, down_buf))
        return [
            pltpu.make_async_copy(src.at[at_layer], dst.at[at_layer % 2], weight_sem.at[at_layer % 2, at])
            for at, (src, dst) in enumerate(pairs)
        ]

    def load_stale(at_layer):
        place = n_layers + at_layer % 2
        return [
            pltpu.make_async_copy(src.at[0, at_layer, peer_rows], kv_peer.at[place, part], stale_sem.at[at_layer % 2, part])
            for part, src in enumerate((k_stale, v_stale))
        ]

    def send_kv(at_layer, target, arrival):
        return [
            pltpu.make_async_remote_copy(
                src_ref=kv_own.at[at_layer, part], dst_ref=target.at[at_layer, part],
                send_sem=send_sem.at[at_layer, part], recv_sem=arrival.at[at_layer, part],
                device_id={"patch": other}, device_id_type=MESH)
            for part in range(2)
        ]

    def send_fresh(at_layer):
        return send_kv(at_layer, kv_peer, recv_sem)

    def send_final(at_layer):
        return send_kv(at_layer, kv_fin.at[1], last_sem)

    def keep_final(at_layer):
        return [
            pltpu.make_async_copy(kv_own.at[at_layer, part], kv_fin.at[0, at_layer, part], keep_sem.at[at_layer, part])
            for part in range(2)
        ]

    def half_rows(half):
        return slice(half * (rows // 2), (half + 1) * (rows // 2))

    def send_eps(at_step, half):
        at = pl.ds(half * (rows // 2), rows // 2)
        return pltpu.make_async_remote_copy(
            src_ref=eps_out.at[at], dst_ref=eps_recv.at[at_step, at],
            send_sem=eps_send_sem.at[half], recv_sem=eps_recv_sem.at[at_step, half],
            device_id={"cfg": partner}, device_id_type=MESH)

    def modulate(at_layer, parts):
        cond = cond_buf[...]
        act = (cond * jax.nn.sigmoid(cond)).astype(BF16)
        for part in parts:
            cols = slice(part * 2 * width, (part + 1) * 2 * width)
            mod_buf[at_layer, 0:n_steps, cols] = jnp.dot(act, ada_buf[at_layer % 2, :, cols], preferred_element_type=F32)

    def block(step, layer):
        side = layer % 2
        wait(load_weights(layer))
        if step == 0:
            wait(load_stale(layer))

            @pl.when(layer + 1 < n_layers)
            def _():
                wait(load_ada(layer + 1))
                start(load_stale(layer + 1))

            @pl.when(layer + 2 < n_layers)
            def _():
                start(load_ada(layer + 2))
        else:
            for copy in send_fresh(layer):
                copy.wait_recv()
                copy.wait_send()
        if step < last_step:
            start(load_weights(lax.rem(layer + 1, n_layers)))
        else:
            @pl.when(layer + 1 < n_layers)
            def _():
                start(load_weights(layer + 1))

        def mod(part):
            return mod_buf[layer, step:step + 1, part * width:(part + 1) * width]

        h = (normed(resid[...]) * (1.0 + mod(1)) + mod(0)).astype(BF16)
        qkv = jnp.dot(h, qkv_buf[side], preferred_element_type=F32).astype(BF16)
        kv_own[layer, 0] = qkv[:, width:2 * width]
        kv_own[layer, 1] = qkv[:, 2 * width:]

        place = n_layers + layer % 2 if step == 0 else layer
        factor = head_dim ** -0.5 * math.log2(math.e)
        pair_width = 2 * head_dim
        lane = lax.broadcasted_iota(jnp.int32, (rows, pair_width), 1)
        tops, totals = {}, {}

        def cols_of(head):
            base = head // 2 * pair_width
            return slice(base, base + pair_width)

        def score(head):
            cols = cols_of(head)
            keep = (lane < head_dim) if head % 2 == 0 else (lane >= head_dim)
            q_head = jnp.where(keep, qkv[:, cols], jnp.zeros((rows, pair_width), BF16))
            top = None
            for side_at, keys in enumerate((kv_own.at[layer, 0], kv_peer.at[place, 0])):
                for base in range(0, rows, 128):
                    s = contract(keys[base:base + 128, cols], q_head, 1, 1)
                    s_buf[head % 3, side_at, base:base + 128] = s
                    folded = jnp.max(s.reshape(128 // 8, 8, rows), 0)
                    top = folded if top is None else jnp.maximum(top, folded)
            top = jnp.max(top, 0, keepdims=True)
            tops[head] = top

        def weigh(head):
            total = None
            for side_at in range(2):
                for base in range(0, rows, 16):
                    e = jnp.exp2((s_buf[head % 3, side_at, base:base + 16] - tops[head]) * factor)
                    p_buf[head % 3, side_at, base:base + 16] = e.astype(BF16)
                    folded = jnp.sum(e.reshape(16 // 8, 8, rows), 0)
                    total = folded if total is None else total + folded
            totals[head] = jnp.sum(total, 0, keepdims=True)

        def mix(head):
            cols = cols_of(head)
            part = slice(head % 2 * head_dim, (head % 2 + 1) * head_dim)
            mixed = None
            for side, values in enumerate((kv_own[layer, 1, :, cols], kv_peer[place, 1, :, cols])):
                term = contract(values.T[part], p_buf[head % 3, side], 1, 0)
                mixed = term if mixed is None else mixed + term
            o_buf[head * head_dim:(head + 1) * head_dim, :] = (mixed * (1.0 / totals[head])).astype(BF16)

        for turn in range(n_heads + 4):
            if turn < n_heads:
                score(turn)
            if 2 <= turn < n_heads + 2:
                weigh(turn - 2)
            if turn >= 4:
                mix(turn - 4)

        attn = contract(o_buf[...], out_buf[side], 0, 0)
        r = resid[...] + mod(2) * attn
        if step == 0:
            modulate(layer + 1, range(3))
        h2 = (normed(r) * (0.5 * (1.0 + mod(4))) + 0.5 * mod(3)).astype(BF16)
        chunk = 256
        starts = list(range(0, up_buf.shape[2], chunk))
        down = None

        def up_half(base):
            return jnp.dot(h2, up_buf[side, :, base:base + chunk], preferred_element_type=F32)

        lag = 2
        halves = [up_half(base) for base in starts[:lag]]
        for at, base in enumerate(starts):
            if at + lag < len(starts):
                halves.append(up_half(starts[at + lag]))
            act = gelu_of_half(halves[at]).astype(BF16)
            term = jnp.dot(act, down_buf[side, base:base + chunk, :], preferred_element_type=F32)
            down = term if down is None else down + term
        resid[...] = r + mod(5) * down
        if step < last_step:
            start(send_fresh(layer))
        else:
            start(send_final(layer) + keep_final(layer))

    barrier = pltpu.get_barrier_semaphore()
    pl.semaphore_signal(barrier, inc=1, device_id={"patch": other}, device_id_type=MESH)
    pl.semaphore_signal(barrier, inc=1, device_id={"cfg": partner}, device_id_type=MESH)
    start(load_small())
    start(load_ada(0))
    start(load_weights(0))
    start(load_stale(0))
    wait(load_small())
    x_out[...] = lat_buf[...].astype(F32)
    resid[...] = lat_buf[...].astype(F32)
    wait(load_ada(0))
    start(load_ada(1))
    modulate(0, range(3))
    pl.semaphore_wait(barrier, 2)

    for step in range(n_steps):
        lax.fori_loop(0, n_layers, lambda layer, carry: (block(step, layer), carry)[1], 0)
        for half in range(2):
            at = half_rows(half)
            if step > 0:
                send_eps(step - 1, half).wait_send()
            eps = jnp.dot(normed(resid[at]).astype(BF16), head_buf[...], preferred_element_type=F32)
            eps_out[at] = eps.astype(BF16)
            if step < last_step:
                send_eps(step, half).start()
        if step < last_step:
            for half in range(2):
                at = half_rows(half)
                send_eps(step, half).wait_recv()
                x_now = guide(slot, sched_ref, step, x_out[at], eps_out[at], eps_recv[step, at])
                x_out[at] = x_now
                resid[at] = x_now

    def drain(at_layer, carry):
        for copy in send_final(at_layer):
            copy.wait_send()
            copy.wait_recv()
        wait(keep_final(at_layer))
        return carry

    lax.fori_loop(0, n_layers, drain, 0)


def guide(slot, sched, step, x, mine, peer):
    mine, peer = mine.astype(F32), peer.astype(F32)
    is_cond = slot % 2 == 0
    eps_cond = jnp.where(is_cond, mine, peer)
    eps_unc = jnp.where(is_cond, peer, mine)
    guided = eps_unc + sched[step, 2] * (eps_cond - eps_unc)
    return sched[step, 0] * x + sched[step, 1] * guided


def store_kernel(kv_fin, k_out, v_out, buf, in_sem, out_sem):
    n_layers, rows = buf.shape[1], buf.shape[3]
    patch = lax.axis_index("patch")
    loads, stores = [], []
    for layer in range(n_layers):
        for side, owner in enumerate((patch, 1 - patch)):
            for part, dst in enumerate((k_out, v_out)):
                at = pl.ds(pl.multiple_of(owner * rows, rows), rows)
                here = buf.at[side, layer, part]
                loads.append(pltpu.make_async_copy(kv_fin.at[side, layer, part], here, in_sem.at[side, layer, part]))
                stores.append(pltpu.make_async_copy(here, dst.at[0, layer, at], out_sem.at[side, layer, part]))
    for copy in loads:
        copy.start()
    for load, store in zip(loads, stores):
        load.wait()
        store.start()
    for copy in stores:
        copy.wait()


def guide_kernel(step, sched_ref, x_ref, mine_ref, peer_ref, x_new):
    x_new[0] = guide(lax.axis_index("cfg"), sched_ref, step, x_ref[...], mine_ref[...], peer_ref[...])


def solution(mesh):
    slot_spec = P(("img", "cfg"), None, None)
    cache_spec = P(("img", "cfg"), None, None, None)
    rep_spec = P()
    n_cfg = mesh.shape["cfg"]
    partner = [(at, at ^ 1) for at in range(n_cfg)]

    def local_step(latent, cond_vec, sched_coef, w_ada, w_qkv, w_out, w_up, w_down, w_head, k_stale, v_stale):
        n_layers, width = w_qkv.shape[0], w_qkv.shape[1]
        rows = latent.shape[1]
        n_heads, head_dim = w_out.shape[1], w_out.shape[2]
        n_steps = sched_coef.shape[1]
        w_out = w_out.reshape(n_layers, width, width)

        any_spec = pl.BlockSpec(memory_space=pl.ANY)
        vmem_spec = pl.BlockSpec(memory_space=pltpu.VMEM)
        kv_shape = (2, n_layers, 2, rows, width)
        x_last, eps, kv_fin = pl.pallas_call(
            functools.partial(kernel, n_steps, n_layers, n_heads, head_dim),
            out_shape=[
                jax.ShapeDtypeStruct((rows, width), F32),
                jax.ShapeDtypeStruct((rows, width), BF16),
                jax.ShapeDtypeStruct(kv_shape, BF16),
            ],
            in_specs=[any_spec] * 11,
            out_specs=[vmem_spec, vmem_spec, any_spec],
            scratch_shapes=[
                pltpu.SMEM(sched_coef.shape[::-1], F32),
                pltpu.VMEM(cond_vec.shape[1:], F32),
                pltpu.VMEM((rows, width), BF16),
                pltpu.VMEM(w_head.shape, BF16),
                pltpu.VMEM((2,) + w_ada.shape[1:], BF16),
                pltpu.VMEM((2,) + w_qkv.shape[1:], BF16),
                pltpu.VMEM((2,) + w_out.shape[1:], BF16),
                pltpu.VMEM((2,) + w_up.shape[1:], BF16),
                pltpu.VMEM((2,) + w_down.shape[1:], BF16),
                pltpu.VMEM((rows, width), F32),
                pltpu.VMEM((n_layers + 1, 8, 6 * width), F32),
                pltpu.VMEM((width, rows), BF16),
                pltpu.VMEM((3, 2, rows, rows), F32),
                pltpu.VMEM((3, 2, rows, rows), BF16),
                pltpu.VMEM((n_layers, 2, rows, width), BF16),
                pltpu.VMEM((n_layers + 2, 2, rows, width), BF16),
                pltpu.VMEM((n_steps, rows, width), BF16),
                pltpu.SemaphoreType.DMA((4,)),
                pltpu.SemaphoreType.DMA((2,)),
                pltpu.SemaphoreType.DMA((2, 4)),
                pltpu.SemaphoreType.DMA((2, 2)),
                pltpu.SemaphoreType.DMA((n_layers, 2)),
                pltpu.SemaphoreType.DMA((n_layers, 2)),
                pltpu.SemaphoreType.DMA((n_layers, 2)),
                pltpu.SemaphoreType.DMA((n_layers, 2)),
                pltpu.SemaphoreType.DMA((2,)),
                pltpu.SemaphoreType.DMA((n_steps, 2)),
            ],
            compiler_params=pltpu.CompilerParams(
                collective_id=0, has_side_effects=True, vmem_limit_bytes=VMEM_ALL,
            ),
            name="denoise",
        )(latent, cond_vec, sched_coef.T, w_ada, w_qkv, w_out, w_up, w_down, w_head, k_stale, v_stale)
        eps_peer = lax.ppermute(eps, "cfg", partner)
        k_new, v_new = pl.pallas_call(
            store_kernel,
            out_shape=[jax.ShapeDtypeStruct(k_stale.shape, BF16), jax.ShapeDtypeStruct(v_stale.shape, BF16)],
            in_specs=[any_spec],
            out_specs=[any_spec] * 2,
            scratch_shapes=[
                pltpu.VMEM(kv_shape, BF16),
                pltpu.SemaphoreType.DMA(kv_shape[:3]),
                pltpu.SemaphoreType.DMA(kv_shape[:3]),
            ],
            compiler_params=pltpu.CompilerParams(vmem_limit_bytes=VMEM_ALL),
            cost_estimate=pl.CostEstimate(flops=0, bytes_accessed=2 * 2 * k_stale.size * 2, transcendentals=0),
            name="store",
        )(kv_fin)
        x_new = pl.pallas_call(
            functools.partial(guide_kernel, n_steps - 1),
            out_shape=jax.ShapeDtypeStruct((1, rows, width), F32),
            in_specs=[pl.BlockSpec(memory_space=pltpu.SMEM)] + [vmem_spec] * 3,
            out_specs=vmem_spec,
            name="guide",
        )(sched_coef.T, x_last, eps, eps_peer)
        return x_new, k_new, v_new

    return jax.shard_map(
        local_step,
        mesh=mesh,
        in_specs=(P("img", "patch", None), slot_spec, rep_spec, rep_spec, rep_spec, rep_spec, rep_spec, rep_spec, rep_spec, cache_spec, cache_spec),
        out_specs=(P(("img", "cfg"), "patch", None), cache_spec, cache_spec),
        check_vma=False,
    )
```

```python
import functools
import math

import jax
import jax.numpy as jnp
from jax import lax
from jax.experimental import pallas as pl
from jax.experimental.pallas import tpu as pltpu
from jax.sharding import PartitionSpec as P

MESH = pl.DeviceIdType.MESH
F32 = jnp.float32
BF16 = jnp.bfloat16
VMEM_ALL = 67043328
GELU_A = math.sqrt(2.0 / math.pi)
GELU_B = GELU_A * 0.044715


def normed(values):
    row_mean = jnp.mean(values, -1, keepdims=True)
    centered = values - row_mean
    row_var = jnp.mean(centered * centered, -1, keepdims=True)
    return centered * lax.rsqrt(row_var + 1e-6)


def gelu_of_half(half):
    return half + half * jnp.tanh(half * (2.0 * GELU_A + 8.0 * GELU_B * (half * half)))


def contract(a, b, a_dim, b_dim):
    return lax.dot_general(a, b, (((a_dim,), (b_dim,)), ((), ())), preferred_element_type=F32)


def kernel(
    n_steps, n_layers, n_heads, head_dim,
    latent_hbm, cond_hbm, sched_hbm, ada_hbm, qkv_hbm, out_hbm, up_hbm, down_hbm, head_hbm, k_stale, v_stale,
    x_out, eps_out, kv_fin,
    sched_ref, cond_buf, lat_buf, head_buf, ada_buf, qkv_buf, out_buf, up_buf, down_buf,
    resid, mod_buf, o_buf, s_buf, p_buf, kv_own, kv_peer, eps_recv,
    small_sem, ada_sem, weight_sem, stale_sem, send_sem, recv_sem, last_sem, keep_sem, eps_send_sem, eps_recv_sem,
):
    rows, width = resid.shape
    patch = lax.axis_index("patch")
    slot = lax.axis_index("cfg")
    other = 1 - patch
    partner = slot + 1 - 2 * (slot % 2)
    peer_rows = pl.ds(pl.multiple_of(other * rows, rows), rows)
    last_step = n_steps - 1

    def start(copies):
        for copy in copies:
            copy.start()

    def wait(copies):
        for copy in copies:
            copy.wait()

    def load_small():
        pairs = ((latent_hbm.at[slot // 2], lat_buf), (cond_hbm.at[0], cond_buf), (sched_hbm, sched_ref), (head_hbm, head_buf))
        return [pltpu.make_async_copy(src, dst, small_sem.at[at]) for at, (src, dst) in enumerate(pairs)]

    def load_ada(at_layer):
        return [pltpu.make_async_copy(ada_hbm.at[at_layer], ada_buf.at[at_layer % 2], ada_sem.at[at_layer % 2])]

    def load_weights(at_layer):
        pairs = ((qkv_hbm, qkv_buf), (out_hbm, out_buf), (up_hbm, up_buf), (down_hbm, down_buf))
        return [
            pltpu.make_async_copy(src.at[at_layer], dst.at[at_layer % 2], weight_sem.at[at_layer % 2, at])
            for at, (src, dst) in enumerate(pairs)
        ]

    def load_stale(at_layer):
        place = n_layers + at_layer % 2
        return [
            pltpu.make_async_copy(src.at[0, at_layer, peer_rows], kv_peer.at[place, part], stale_sem.at[at_layer % 2, part])
            for part, src in enumerate((k_stale, v_stale))
        ]

    def send_kv(at_layer, target, arrival):
        return [
            pltpu.make_async_remote_copy(
                src_ref=kv_own.at[at_layer, part], dst_ref=target.at[at_layer, part],
                send_sem=send_sem.at[at_layer, part], recv_sem=arrival.at[at_layer, part],
                device_id={"patch": other}, device_id_type=MESH)
            for part in range(2)
        ]

    def send_fresh(at_layer):
        return send_kv(at_layer, kv_peer, recv_sem)

    def send_final(at_layer):
        return send_kv(at_layer, kv_fin.at[1], last_sem)

    def keep_final(at_layer):
        return [
            pltpu.make_async_copy(kv_own.at[at_layer, part], kv_fin.at[0, at_layer, part], keep_sem.at[at_layer, part])
            for part in range(2)
        ]

    def half_rows(half):
        return slice(half * (rows // 2), (half + 1) * (rows // 2))

    def send_eps(at_step, half):
        at = pl.ds(half * (rows // 2), rows // 2)
        return pltpu.make_async_remote_copy(
            src_ref=eps_out.at[at], dst_ref=eps_recv.at[at_step, at],
            send_sem=eps_send_sem.at[half], recv_sem=eps_recv_sem.at[at_step, half],
            device_id={"cfg": partner}, device_id_type=MESH)

    def modulate(at_layer, parts):
        cond = cond_buf[...]
        act = (cond * jax.nn.sigmoid(cond)).astype(BF16)
        for part in parts:
            cols = slice(part * 2 * width, (part + 1) * 2 * width)
            mod_buf[at_layer, 0:n_steps, cols] = jnp.dot(act, ada_buf[at_layer % 2, :, cols], preferred_element_type=F32)

    def block(step, layer):
        side = layer % 2
        wait(load_weights(layer))
        if step == 0:
            wait(load_stale(layer))

            @pl.when(layer + 1 < n_layers)
            def _():
                wait(load_ada(layer + 1))
                start(load_stale(layer + 1))

            @pl.when(layer + 2 < n_layers)
            def _():
                start(load_ada(layer + 2))
        else:
            for copy in send_fresh(layer):
                copy.wait_recv()
                copy.wait_send()
        if step < last_step:
            start(load_weights(lax.rem(layer + 1, n_layers)))
        else:
            @pl.when(layer + 1 < n_layers)
            def _():
                start(load_weights(layer + 1))

        def mod(part):
            return mod_buf[layer, step:step + 1, part * width:(part + 1) * width]

        h = (normed(resid[...]) * (1.0 + mod(1)) + mod(0)).astype(BF16)
        qkv = jnp.dot(h, qkv_buf[side], preferred_element_type=F32).astype(BF16)
        kv_own[layer, 0] = qkv[:, width:2 * width]
        kv_own[layer, 1] = qkv[:, 2 * width:]

        place = n_layers + layer % 2 if step == 0 else layer
        factor = head_dim ** -0.5 * math.log2(math.e)
        pair_width = 2 * head_dim
        lane = lax.broadcasted_iota(jnp.int32, (rows, pair_width), 1)
        tops, totals = {}, {}

        def cols_of(head):
            base = head // 2 * pair_width
            return slice(base, base + pair_width)

        def score(head):
            cols = cols_of(head)
            keep = (lane < head_dim) if head % 2 == 0 else (lane >= head_dim)
            q_head = jnp.where(keep, qkv[:, cols], jnp.zeros((rows, pair_width), BF16))
            top = None
            for side_at, keys in enumerate((kv_own.at[layer, 0], kv_peer.at[place, 0])):
                for base in range(0, rows, 128):
                    s = contract(keys[base:base + 128, cols], q_head, 1, 1)
                    s_buf[head % 3, side_at, base:base + 128] = s
                    folded = jnp.max(s.reshape(128 // 8, 8, rows), 0)
                    top = folded if top is None else jnp.maximum(top, folded)
            top = jnp.max(top, 0, keepdims=True)
            tops[head] = top

        def weigh(head):
            total = None
            for side_at in range(2):
                for base in range(0, rows, 16):
                    e = jnp.exp2((s_buf[head % 3, side_at, base:base + 16] - tops[head]) * factor)
                    p_buf[head % 3, side_at, base:base + 16] = e.astype(BF16)
                    folded = jnp.sum(e.reshape(16 // 8, 8, rows), 0)
                    total = folded if total is None else total + folded
            totals[head] = jnp.sum(total, 0, keepdims=True)

        def mix(head):
            cols = cols_of(head)
            part = slice(head % 2 * head_dim, (head % 2 + 1) * head_dim)
            mixed = None
            for side, values in enumerate((kv_own[layer, 1, :, cols], kv_peer[place, 1, :, cols])):
                term = contract(values.T[part], p_buf[head % 3, side], 1, 0)
                mixed = term if mixed is None else mixed + term
            o_buf[head * head_dim:(head + 1) * head_dim, :] = (mixed * (1.0 / totals[head])).astype(BF16)

        for turn in range(n_heads + 4):
            if turn < n_heads:
                score(turn)
            if 2 <= turn < n_heads + 2:
                weigh(turn - 2)
            if turn >= 4:
                mix(turn - 4)

        attn = contract(o_buf[...], out_buf[side], 0, 0)
        r = resid[...] + mod(2) * attn
        if step == 0:
            modulate(layer + 1, range(3))
        h2 = (normed(r) * (0.5 * (1.0 + mod(4))) + 0.5 * mod(3)).astype(BF16)
        chunk = 256
        starts = list(range(0, up_buf.shape[2], chunk))
        down = None

        def up_half(base):
            return jnp.dot(h2, up_buf[side, :, base:base + chunk], preferred_element_type=F32)

        lag = 2
        halves = [up_half(base) for base in starts[:lag]]
        for at, base in enumerate(starts):
            if at + lag < len(starts):
                halves.append(up_half(starts[at + lag]))
            act = gelu_of_half(halves[at]).astype(BF16)
            term = jnp.dot(act, down_buf[side, base:base + chunk, :], preferred_element_type=F32)
            down = term if down is None else down + term
        resid[...] = r + mod(5) * down
        if step < last_step:
            start(send_fresh(layer))
        else:
            start(send_final(layer) + keep_final(layer))

    barrier = pltpu.get_barrier_semaphore()
    pl.semaphore_signal(barrier, inc=1, device_id={"patch": other}, device_id_type=MESH)
    pl.semaphore_signal(barrier, inc=1, device_id={"cfg": partner}, device_id_type=MESH)
    start(load_small())
    start(load_ada(0))
    start(load_weights(0))
    start(load_stale(0))
    wait(load_small())
    x_out[...] = lat_buf[...].astype(F32)
    resid[...] = lat_buf[...].astype(F32)
    wait(load_ada(0))
    start(load_ada(1))
    modulate(0, range(3))
    pl.semaphore_wait(barrier, 2)

    for step in range(n_steps):
        def two(at, carry, step=step):
            block(step, 2 * at)
            block(step, 2 * at + 1)
            return carry

        lax.fori_loop(0, n_layers // 2, two, 0)
        for half in range(2):
            at = half_rows(half)
            if step > 0:
                send_eps(step - 1, half).wait_send()
            eps = jnp.dot(normed(resid[at]).astype(BF16), head_buf[...], preferred_element_type=F32)
            eps_out[at] = eps.astype(BF16)
            if step < last_step:
                send_eps(step, half).start()
        if step < last_step:
            for half in range(2):
                at = half_rows(half)
                send_eps(step, half).wait_recv()
                x_now = guide(slot, sched_ref, step, x_out[at], eps_out[at], eps_recv[step, at])
                x_out[at] = x_now
                resid[at] = x_now

    def drain(at_layer, carry):
        for copy in send_final(at_layer):
            copy.wait_send()
            copy.wait_recv()
        wait(keep_final(at_layer))
        return carry

    lax.fori_loop(0, n_layers, drain, 0)


def guide(slot, sched, step, x, mine, peer):
    mine, peer = mine.astype(F32), peer.astype(F32)
    is_cond = slot % 2 == 0
    eps_cond = jnp.where(is_cond, mine, peer)
    eps_unc = jnp.where(is_cond, peer, mine)
    guided = eps_unc + sched[step, 2] * (eps_cond - eps_unc)
    return sched[step, 0] * x + sched[step, 1] * guided


def store_kernel(kv_fin, k_out, v_out, buf, in_sem, out_sem):
    n_layers, rows = buf.shape[1], buf.shape[3]
    patch = lax.axis_index("patch")
    loads, stores = [], []
    for layer in range(n_layers):
        for side, owner in enumerate((patch, 1 - patch)):
            for part, dst in enumerate((k_out, v_out)):
                at = pl.ds(pl.multiple_of(owner * rows, rows), rows)
                here = buf.at[side, layer, part]
                loads.append(pltpu.make_async_copy(kv_fin.at[side, layer, part], here, in_sem.at[side, layer, part]))
                stores.append(pltpu.make_async_copy(here, dst.at[0, layer, at], out_sem.at[side, layer, part]))
    for copy in loads:
        copy.start()
    for load, store in zip(loads, stores):
        load.wait()
        store.start()
    for copy in stores:
        copy.wait()


def guide_kernel(step, sched_ref, x_ref, mine_ref, peer_ref, x_new):
    x_new[0] = guide(lax.axis_index("cfg"), sched_ref, step, x_ref[...], mine_ref[...], peer_ref[...])


def solution(mesh):
    slot_spec = P(("img", "cfg"), None, None)
    cache_spec = P(("img", "cfg"), None, None, None)
    rep_spec = P()
    n_cfg = mesh.shape["cfg"]
    partner = [(at, at ^ 1) for at in range(n_cfg)]

    def local_step(latent, cond_vec, sched_coef, w_ada, w_qkv, w_out, w_up, w_down, w_head, k_stale, v_stale):
        n_layers, width = w_qkv.shape[0], w_qkv.shape[1]
        rows = latent.shape[1]
        n_heads, head_dim = w_out.shape[1], w_out.shape[2]
        n_steps = sched_coef.shape[1]
        w_out = w_out.reshape(n_layers, width, width)

        any_spec = pl.BlockSpec(memory_space=pl.ANY)
        vmem_spec = pl.BlockSpec(memory_space=pltpu.VMEM)
        kv_shape = (2, n_layers, 2, rows, width)
        x_last, eps, kv_fin = pl.pallas_call(
            functools.partial(kernel, n_steps, n_layers, n_heads, head_dim),
            out_shape=[
                jax.ShapeDtypeStruct((rows, width), F32),
                jax.ShapeDtypeStruct((rows, width), BF16),
                jax.ShapeDtypeStruct(kv_shape, BF16),
            ],
            in_specs=[any_spec] * 11,
            out_specs=[vmem_spec, vmem_spec, any_spec],
            scratch_shapes=[
                pltpu.SMEM(sched_coef.shape[::-1], F32),
                pltpu.VMEM(cond_vec.shape[1:], F32),
                pltpu.VMEM((rows, width), BF16),
                pltpu.VMEM(w_head.shape, BF16),
                pltpu.VMEM((2,) + w_ada.shape[1:], BF16),
                pltpu.VMEM((2,) + w_qkv.shape[1:], BF16),
                pltpu.VMEM((2,) + w_out.shape[1:], BF16),
                pltpu.VMEM((2,) + w_up.shape[1:], BF16),
                pltpu.VMEM((2,) + w_down.shape[1:], BF16),
                pltpu.VMEM((rows, width), F32),
                pltpu.VMEM((n_layers + 1, 8, 6 * width), F32),
                pltpu.VMEM((width, rows), BF16),
                pltpu.VMEM((3, 2, rows, rows), F32),
                pltpu.VMEM((3, 2, rows, rows), BF16),
                pltpu.VMEM((n_layers, 2, rows, width), BF16),
                pltpu.VMEM((n_layers + 2, 2, rows, width), BF16),
                pltpu.VMEM((n_steps, rows, width), BF16),
                pltpu.SemaphoreType.DMA((4,)),
                pltpu.SemaphoreType.DMA((2,)),
                pltpu.SemaphoreType.DMA((2, 4)),
                pltpu.SemaphoreType.DMA((2, 2)),
                pltpu.SemaphoreType.DMA((n_layers, 2)),
                pltpu.SemaphoreType.DMA((n_layers, 2)),
                pltpu.SemaphoreType.DMA((n_layers, 2)),
                pltpu.SemaphoreType.DMA((n_layers, 2)),
                pltpu.SemaphoreType.DMA((2,)),
                pltpu.SemaphoreType.DMA((n_steps, 2)),
            ],
            compiler_params=pltpu.CompilerParams(
                collective_id=0, has_side_effects=True, vmem_limit_bytes=62 * 1024 * 1024,
            ),
            name="denoise",
        )(latent, cond_vec, sched_coef.T, w_ada, w_qkv, w_out, w_up, w_down, w_head, k_stale, v_stale)
        eps_peer = lax.ppermute(eps, "cfg", partner)
        k_new, v_new = pl.pallas_call(
            store_kernel,
            out_shape=[jax.ShapeDtypeStruct(k_stale.shape, BF16), jax.ShapeDtypeStruct(v_stale.shape, BF16)],
            in_specs=[any_spec],
            out_specs=[any_spec] * 2,
            scratch_shapes=[
                pltpu.VMEM(kv_shape, BF16),
                pltpu.SemaphoreType.DMA(kv_shape[:3]),
                pltpu.SemaphoreType.DMA(kv_shape[:3]),
            ],
            compiler_params=pltpu.CompilerParams(vmem_limit_bytes=62 * 1024 * 1024),
            cost_estimate=pl.CostEstimate(flops=0, bytes_accessed=2 * 2 * k_stale.size * 2, transcendentals=0),
            name="store",
        )(kv_fin)
        x_new = pl.pallas_call(
            functools.partial(guide_kernel, n_steps - 1),
            out_shape=jax.ShapeDtypeStruct((1, rows, width), F32),
            in_specs=[pl.BlockSpec(memory_space=pltpu.SMEM)] + [vmem_spec] * 3,
            out_specs=vmem_spec,
            compiler_params=pltpu.CompilerParams(vmem_limit_bytes=8 * 1024 * 1024),
            name="guide",
        )(sched_coef.T, x_last, eps, eps_peer)
        return x_new, k_new, v_new

    return jax.shard_map(
        local_step,
        mesh=mesh,
        in_specs=(P("img", "patch", None), slot_spec, rep_spec, rep_spec, rep_spec, rep_spec, rep_spec, rep_spec, rep_spec, cache_spec, cache_spec),
        out_specs=(P(("img", "cfg"), "patch", None), cache_spec, cache_spec),
        check_vma=False,
    )
```
